32 devices in a mesh: section: 4 (over z), tensor: 8 (over y, x, core).
Axes of the slice: x: 2, y: 2, z: 4, core: 2. Of those that a mesh axis runs over, the one named last changes fastest.
Arguments:
- hidden_state: bfloat16 [64, 8192], P('section'), may hold values from -6 to 6
- norm_gain: float32 [8192], replicated, may hold values from 0.5 to 1.5
- wq_old: bfloat16 [8192, 8192], P('section', 'tensor'), may hold values from -0.0625 to 0.0625
- wkv_old: bfloat16 [8192, 2048], P('tensor', 'section'), may hold values from -0.0625 to 0.0625
- kv_old: bfloat16 [8, 4096, 16, 256], P('section', 'tensor'), may hold values from -241 to 241
- page_table: int32 [64, 64], replicated, may hold values from 0 to 4095, as said below
- lengths: int32 [64], replicated, may hold values from 1 to 1023
Outputs:
- context: bfloat16 [64, 8192], P('section', 'tensor')
- kv_new: bfloat16 [64, 8, 1024, 256], P('section', 'tensor')
- wq_new: bfloat16 [8192, 8192], P(None, 'tensor')
- wkv_new: bfloat16 [8192, 2048], P(None, 'tensor')
The draws below stay inside these ranges and needn't reach their ends.
Inputs may be any that keep to these rules, and one draw needn't show every extreme that they name: `page_table`: every pool page belongs to exactly one page of one request. Each block of 512 consecutive pool pages holds exactly 8 pages of every request.
All inputs are finite; a program needn't handle non-finite values.
Results may differ from the reference program's by a relative error of at most 0.0075.
The reference program's roundings to bfloat16 on the way (of `normed`, `fresh`, `cache` and `probs`) count: a program that leaves them out, or rounds other values in their place, can miss the bound.
Values may be sent and summed in bfloat16 or wider, within the bound.
A program may use at most 128 MiB of HBM per device.

```python
import jax
import jax.numpy as jnp
from jax import lax

D = 8192
HEADS = 64
KV_HEADS = 8
HEAD_DIM = 128
PAGE = 16
REQS = 64
MAXPAGES = 64
SLOTS = 1024
POOL = 4096
POOL_BLOCKS = 8
KV_COPIES = 8


def draw_page_table(key, part):
    per_block = MAXPAGES // POOL_BLOCKS
    pool_dev = POOL // POOL_BLOCKS
    slot_keys = jax.random.split(jax.random.fold_in(key, 11), REQS)
    orders = jax.vmap(lambda item: jax.random.permutation(item, MAXPAGES))(slot_keys)
    block = orders // per_block
    within = orders % per_block
    block_keys = jax.random.split(jax.random.fold_in(key, 12), POOL_BLOCKS)
    spots = jax.vmap(lambda item: jax.random.permutation(item, pool_dev))(block_keys)
    request = jnp.arange(REQS, dtype=jnp.int32)[:, None]
    local = spots[block, request * per_block + within]
    return (block * pool_dev + local).astype(jnp.int32)


def draw_kv_old(key, part):
    shape = (KV_HEADS, POOL, PAGE, 2 * HEAD_DIM)
    base = jnp.clip(jax.random.normal(jax.random.fold_in(key, 21), shape, jnp.float32), -6.0, 6.0)
    return base.astype(jnp.bfloat16)


def touch_ends(drawn, stream_key, low, top_value):
    shape = drawn.shape
    spot = [jax.random.randint(jax.random.fold_in(stream_key, axis), (), 0, shape[axis]) for axis in range(len(shape))]
    drawn = drawn.at[tuple(spot)].set(low)
    longest = shape.index(max(shape))
    spot[longest] = (spot[longest] + 1) % shape[longest]
    return drawn.at[tuple(spot)].set(top_value)


def shard_levels(own_key, dims, cuts, smallest, top_value):
    gain, own = 1.0, jax.random.fold_in(own_key, 6)
    for dim, shards_of in cuts:
        draws = jnp.exp(jax.random.uniform(jax.random.fold_in(own, dim), (shards_of,), jnp.float32, smallest / len(cuts), top_value / len(cuts)))
        gain = gain * jnp.repeat(draws, dims[dim] // shards_of).reshape([-1 if axis == dim else 1 for axis in range(len(dims))])
    return gain


def centred(own_key, extent, deviation, most, cuts=(), kind=jnp.bfloat16):
    values = jax.random.normal(own_key, extent, jnp.float32) * deviation
    if len(cuts) > 0:
        values = shard_levels(own_key, extent, cuts, -0.22, 0.18) * values
    return jnp.clip(values, min=-most, max=most).astype(kind)


def setup_inputs(seed: int = 0) -> dict:
    key_of = jax.random.split(jax.random.key(seed), 8)
    hidden_state = centred(key_of[0], (REQS, D), 1.0, 6.0, ((0, 4),))
    norm_gain = jnp.clip(1.0 + 0.1 * jax.random.normal(key_of[1], (D,), jnp.float32), 0.5, 1.5)
    wq_old = centred(key_of[2], (D, HEADS * HEAD_DIM), D ** -0.5, 0.0625, ((0, 4), (1, 8)))
    wkv_old = centred(key_of[3], (D, KV_HEADS * 2 * HEAD_DIM), D ** -0.5, 0.0625, ((0, 8), (1, 4)))
    kv_old = draw_kv_old(jax.random.fold_in(key_of[7], 71), 0)
    page_table = draw_page_table(jax.random.fold_in(key_of[7], 71), 0)
    lengths = touch_ends(jax.random.randint(key_of[6], (REQS,), 1, SLOTS), jax.random.fold_in(key_of[6], 1), 1, SLOTS - 1).astype(jnp.int32)
    return {"hidden_state": hidden_state, "norm_gain": norm_gain, "wq_old": wq_old, "wkv_old": wkv_old, "kv_old": kv_old, "page_table": page_table, "lengths": lengths}


EPSILON = 1e-05
ROPE_BASE = 500000.0

def rotate(values, position, head_dim):
    half = head_dim // 2
    frequency = ROPE_BASE ** (-(jnp.arange(half, dtype=jnp.float32) * 2.0 / head_dim))
    angles = position.astype(jnp.float32)[:, None] * frequency[None, :]
    cosine = jnp.cos(angles)[:, None, :]
    sine = jnp.sin(angles)[:, None, :]
    first = values[..., :half]
    second = values[..., half:]
    return jnp.concatenate([first * cosine - second * sine, second * cosine + first * sine], axis=-1)

def reference(hidden_state, norm_gain, wq_old, wkv_old, kv_old, page_table, lengths):
    width = 2 * HEAD_DIM
    group = HEADS // KV_HEADS
    repeats = KV_COPIES // KV_HEADS
    widened = hidden_state.astype(jnp.float32)
    scale = lax.rsqrt(lax.optimization_barrier(jnp.mean(widened * widened, axis=1, keepdims=True)) + EPSILON)
    normed = (widened * scale * norm_gain.astype(jnp.float32)).astype(jnp.bfloat16)
    query = jnp.dot(normed, wq_old, preferred_element_type=jnp.float32).reshape(REQS, HEADS, HEAD_DIM)
    query = rotate(query, lengths, HEAD_DIM).astype(jnp.bfloat16)
    fresh = jnp.dot(normed, wkv_old, preferred_element_type=jnp.float32).reshape(REQS, KV_HEADS, width)
    fresh_key = rotate(fresh[:, :, :HEAD_DIM], lengths, HEAD_DIM)
    fresh = jnp.concatenate([fresh_key, fresh[:, :, HEAD_DIM:]], axis=2).astype(jnp.bfloat16)
    slot_ids = jnp.arange(SLOTS, dtype=jnp.int32)
    written = slot_ids[None, :] == lengths[:, None]
    visible = slot_ids[None, :] <= lengths[:, None]

    def per_head(head):
        pages = kv_old[head][page_table]
        cache = pages.reshape(REQS, SLOTS, width)
        token = lax.dynamic_index_in_dim(fresh, head, 1, keepdims=False)
        cache = jnp.where(written[:, :, None], token[:, None, :], cache)
        queries = lax.dynamic_slice_in_dim(query, head * group, group, 1).astype(jnp.float32)
        scores = jnp.einsum('rgd,rsd->rgs', queries, cache[:, :, :HEAD_DIM].astype(jnp.float32)) * HEAD_DIM ** (-0.5)
        seen = visible[:, None, :]
        peak = lax.optimization_barrier(jnp.max(jnp.where(seen, scores, -jnp.inf), axis=2, keepdims=True))
        weights = jnp.where(seen, jnp.exp(scores - peak), 0.0)
        probs = (weights / lax.optimization_barrier(jnp.sum(weights, axis=2, keepdims=True))).astype(jnp.bfloat16)
        mixed = jnp.einsum('rgs,rsd->rgd', probs.astype(jnp.float32), cache[:, :, HEAD_DIM:].astype(jnp.float32))
        return (cache, mixed.astype(jnp.bfloat16))
    caches, mixed = lax.map(per_head, jnp.arange(KV_HEADS, dtype=jnp.int32))
    context = jnp.moveaxis(mixed, 0, 1).reshape(REQS, HEADS * HEAD_DIM)
    kv_new = jnp.repeat(jnp.moveaxis(caches, 0, 1), repeats, axis=1)
    wkv_new = jnp.repeat(wkv_old.reshape(D, KV_HEADS, width), repeats, axis=1).reshape(D, KV_COPIES * width)
    return (context, kv_new, wq_old, wkv_new)
```

```python
import functools

import jax
import jax.numpy as jnp
from jax import lax
from jax.experimental import pallas as pl
from jax.experimental.pallas import tpu as pltpu
from jax.sharding import PartitionSpec as P

KV_HEADS = 8
HEAD_DIM = 128


EPSILON = 1e-05
ROPE_BASE = 500000.0
MESH = pl.DeviceIdType.MESH
CHUNKS = 8


def rotate(values, position, head_dim):
    half = head_dim // 2
    frequency = ROPE_BASE ** (-(jnp.arange(half, dtype=jnp.float32) * 2.0 / head_dim))
    angles = position.astype(jnp.float32)[:, None] * frequency[None, :]
    cosine = jnp.cos(angles)[:, None, :]
    sine = jnp.sin(angles)[:, None, :]
    first = values[..., :half]
    second = values[..., half:]
    return jnp.concatenate(
        [first * cosine - second * sine, second * cosine + first * sine], axis=-1
    )


def pick_kernel(count, spots_ref, kv_ref, out_ref):
    base = pl.program_id(1) * count

    def step(i, carry):
        out_ref[0, 0, i] = kv_ref[0, spots_ref[base + i]]
        return carry

    lax.fori_loop(0, count, step, 0, unroll=8)


def pick_pages(kv_old, spots, sections):
    heads, pool, page, width = kv_old.shape
    count = spots.shape[0] // sections
    return pl.pallas_call(
        functools.partial(pick_kernel, count),
        out_shape=jax.ShapeDtypeStruct((sections, heads, count, page, width), kv_old.dtype),
        grid_spec=pltpu.PrefetchScalarGridSpec(
            num_scalar_prefetch=1,
            grid=(heads, sections),
            in_specs=[pl.BlockSpec((1, pool, page, width), lambda h, s, spots: (h, 0, 0, 0))],
            out_specs=pl.BlockSpec(
                (1, 1, count, page, width), lambda h, s, spots: (s, h, 0, 0, 0)
            ),
        ),
        compiler_params=pltpu.CompilerParams(vmem_limit_bytes=40 * 2**20),
        name="pick_pages",
    )(spots, kv_old)


def exchange_kernel(
    sections,
    tensors,
    local_heads,
    repeats,
    normed_ref,
    wq_ref,
    pages_ref,
    wkv_ref,
    query_ref,
    arrived_ref,
    wkv_new_ref,
    wq_new_ref,
    stage_ref,
    stage_wkv_ref,
    spread,
    part,
    partial_in,
    spread_send,
    spread_recv,
    part_send,
    part_recv,
    page_send,
    page_recv,
    wkv_send,
    wkv_recv,
    local_sem,
    own_send,
    relay_send,
    wq_recv,
    stage_send,
    stage_recv,
):
    me = lax.axis_index("section")
    mine = lax.axis_index("tensor")
    depth, columns = wq_ref.shape
    width = wkv_new_ref.shape[1]
    block = wkv_ref.shape[0]

    def spread_copy(other, slot):
        return pltpu.make_async_remote_copy(
            normed_ref.at[:, pl.ds(pl.multiple_of(other * depth, 128), depth)],
            spread.at[me],
            spread_send.at[slot],
            spread_recv.at[me],
            device_id=(other, mine),
            device_id_type=MESH,
        )

    def part_copy(other, slot):
        return pltpu.make_async_remote_copy(
            part.at[other],
            partial_in.at[me],
            part_send.at[slot],
            part_recv.at[me],
            device_id=(other, mine),
            device_id_type=MESH,
        )

    chunks = own_send.shape[1]
    chunk = depth // chunks

    def wq_rows(owner, i):
        return wq_new_ref.at[pl.ds(pl.multiple_of(owner * depth + i * chunk, 16), chunk), :]

    def own_copy(side, i):
        return pltpu.make_async_remote_copy(
            wq_ref.at[pl.ds(pl.multiple_of(i * chunk, 16), chunk), :],
            wq_rows(me, i),
            own_send.at[side, i],
            wq_recv.at[me, i],
            device_id=(me + (1, -1)[side], mine),
            device_id_type=MESH,
        )

    def relay_copy(owner, side, i):
        return pltpu.make_async_remote_copy(
            wq_rows(owner, i),
            wq_rows(owner, i),
            relay_send.at[owner, i],
            wq_recv.at[owner, i],
            device_id=(me + (1, -1)[side], mine),
            device_id_type=MESH,
        )

    onward = (me + 1 < sections, me > 0)

    def each_chunk(act):
        def run(i, carry):
            act(i)
            return carry

        lax.fori_loop(0, chunks, run, 0)

    for step in range(1, sections):
        spread_copy(lax.rem(me + step, sections), step).start()

    def send_own(i):
        for side in range(2):
            pl.when(onward[side])(lambda: own_copy(side, i).start())

    def stage_copy(origin, other, step, which):
        pairs = (
            (pages_ref.at[other], stage_ref.at[origin]),
            (wkv_ref, stage_wkv_ref.at[origin]),
        )
        return pltpu.make_async_remote_copy(
            *pairs[which],
            stage_send.at[which, step],
            stage_recv.at[which, origin],
            device_id=(other, mine),
            device_id_type=MESH,
        )

    for step in range(1, sections):
        for which in range(2):
            stage_copy(me, lax.rem(me + step, sections), step, which).start()
    each_chunk(send_own)
    keep = pltpu.make_async_copy(
        wq_ref, wq_new_ref.at[pl.ds(pl.multiple_of(me * depth, 16), depth), :], local_sem.at[2]
    )
    keep.start()
    spread[me] = normed_ref[:, pl.ds(pl.multiple_of(me * depth, 128), depth)]

    def page_copy(step, head, copy):
        slot = (step * local_heads + head) * repeats + copy
        other = lax.rem(me + step, sections)
        target = (other * local_heads + head) * repeats + copy
        source = pages_ref.at[me, head] if step == 0 else stage_ref.at[other, head]
        here = (source, arrived_ref.at[mine])
        remote = pltpu.make_async_remote_copy(
            *here,
            page_send.at[slot],
            page_recv.at[mine],
            device_id=(me, target),
            device_id_type=MESH,
        )
        return target, remote, pltpu.make_async_copy(*here, local_sem.at[0])

    def wkv_copy(step, head, copy):
        slot = (step * local_heads + head) * repeats + copy
        other = lax.rem(me + step, sections)
        target = (other * local_heads + head) * repeats + copy
        here = (
            (wkv_ref if step == 0 else stage_wkv_ref.at[other]).at[:, pl.ds(head * width, width)],
            wkv_new_ref.at[pl.ds(pl.multiple_of(mine * block, 128), block), :],
        )
        remote = pltpu.make_async_remote_copy(
            *here,
            wkv_send.at[slot],
            wkv_recv.at[mine],
            device_id=(me, target),
            device_id_type=MESH,
        )
        return target, remote, pltpu.make_async_copy(*here, local_sem.at[1])

    every = [
        (make, step % sections, head, copy)
        for make in (page_copy, wkv_copy)
        for step in range(1, sections + 1)
        for head in range(local_heads)
        for copy in range(repeats)
    ]
    def begin(chosen):
        for make, step, head, copy in every:
            if step == chosen:
                target, remote, local = make(step, head, copy)
                pl.when(target != mine)(remote.start)
                pl.when(target == mine)(local.start)

    begin(0)

    for step in range(1, sections):
        other = lax.rem(me + step, sections)
        spread_copy(other, step).wait_send()
        pltpu.make_async_remote_copy(
            spread.at[other],
            spread.at[other],
            spread_send.at[step],
            spread_recv.at[other],
            device_id=(other, mine),
            device_id_type=MESH,
        ).wait_recv()

    tile = 256

    def product(i, carry):
        group = i // (columns // tile)
        span = pl.ds(pl.multiple_of(lax.rem(i, columns // tile) * tile, tile), tile)
        part[group, :, span] = jnp.dot(
            spread[group], wq_ref[:, span], preferred_element_type=jnp.float32
        )
        return carry

    lax.fori_loop(0, sections * (columns // tile), product, 0)
    for step in range(1, sections):
        part_copy(lax.rem(me + step, sections), step).start()
    partial_in[me] = part[me]

    for step in range(1, sections):
        other = lax.rem(me + step, sections)
        for which in range(2):
            stage_copy(me, other, step, which).wait_send()
            stage_copy(other, other, step, which).wait_recv()
        begin(step)

    for step in range(1, sections):

        def pass_on(i):
            for side in range(2):
                owner = me - step if side == 0 else me + step
                real = owner >= 0 if side == 0 else owner < sections

                @pl.when(real)
                def _():
                    relay_copy(owner, side, i).wait_recv()
                    pl.when(onward[side])(lambda: relay_copy(owner, side, i).start())

        each_chunk(pass_on)

    for step in range(1, sections):
        other = lax.rem(me + step, sections)
        part_copy(other, step).wait_send()
        pltpu.make_async_remote_copy(
            part.at[other],
            partial_in.at[other],
            part_send.at[step],
            part_recv.at[other],
            device_id=(other, mine),
            device_id_type=MESH,
        ).wait_recv()
    total = partial_in[0]
    for group in range(1, sections):
        total = total + partial_in[group]
    query_ref[...] = total

    keep.wait()

    def sent(i):
        for side in range(2):
            pl.when(onward[side])(lambda: own_copy(side, i).wait_send())
            for step in range(1, sections):
                owner = me - step if side == 0 else me + step
                real = owner >= 0 if side == 0 else owner < sections
                pl.when(jnp.logical_and(real, onward[side]))(
                    lambda: relay_copy(owner, side, i).wait_send()
                )

    each_chunk(sent)
    for make, step, head, copy in every:
        target, remote, local = make(step, head, copy)
        pl.when(target != mine)(remote.wait_send)
        pl.when(target == mine)(local.wait)
    for origin in range(tensors):
        pages_in = pltpu.make_async_remote_copy(
            pages_ref.at[0, 0],
            arrived_ref.at[origin],
            page_send.at[0],
            page_recv.at[origin],
            device_id=(me, origin),
            device_id_type=MESH,
        )
        wkv_in = pltpu.make_async_remote_copy(
            wkv_ref.at[:, pl.ds(0, width)],
            wkv_new_ref.at[pl.ds(origin * block, block), :],
            wkv_send.at[0],
            wkv_recv.at[origin],
            device_id=(me, origin),
            device_id_type=MESH,
        )
        outside = mine != origin
        pl.when(outside)(pages_in.wait_recv)
        pl.when(outside)(wkv_in.wait_recv)


def exchange(normed, wq_old, pages, wkv_old, sections, tensors, repeats):
    rows = normed.shape[0]
    depth, columns = wq_old.shape
    local_heads = pages.shape[1]
    width = pages.shape[4]
    copies = sections * local_heads * repeats
    dma = pltpu.SemaphoreType.DMA
    vmem = pl.BlockSpec(memory_space=pltpu.VMEM)
    hbm = pl.BlockSpec(memory_space=pl.ANY)
    return pl.pallas_call(
        functools.partial(exchange_kernel, sections, tensors, local_heads, repeats),
        out_shape=(
            jax.ShapeDtypeStruct((rows, columns), jnp.float32),
            jax.ShapeDtypeStruct((tensors,) + pages.shape[2:], pages.dtype),
            jax.ShapeDtypeStruct((wkv_old.shape[0] * tensors, width), wkv_old.dtype),
            jax.ShapeDtypeStruct((depth * sections, columns), wq_old.dtype),
            jax.ShapeDtypeStruct(pages.shape, pages.dtype),
            jax.ShapeDtypeStruct((sections,) + wkv_old.shape, wkv_old.dtype),
        ),
        in_specs=[vmem, vmem, hbm, hbm],
        out_specs=(vmem, hbm, hbm, hbm, hbm, hbm),
        scratch_shapes=[
            pltpu.VMEM((sections, rows, depth), normed.dtype),
            pltpu.VMEM((sections, rows, columns), jnp.float32),
            pltpu.VMEM((sections, rows, columns), jnp.float32),
            dma((sections,)),
            dma((sections,)),
            dma((sections,)),
            dma((sections,)),
            dma((copies,)),
            dma((tensors,)),
            dma((copies,)),
            dma((tensors,)),
            dma((3,)),
            dma((2, CHUNKS)),
            dma((sections, CHUNKS)),
            dma((sections, CHUNKS)),
            dma((2, sections)),
            dma((2, sections)),
        ],
        compiler_params=pltpu.CompilerParams(
            has_side_effects=True, vmem_limit_bytes=40 * 2**20
        ),
        cost_estimate=pl.CostEstimate(
            flops=2 * sections * rows * depth * columns,
            bytes_accessed=400 * 2**20,
            transcendentals=0,
        ),
        name="exchange",
    )(normed, wq_old, pages, wkv_old)


def attend_kernel(
    pages_of, per_block, page, head_dim, place_ref, length_ref, in_ref, fresh_ref, query_ref, cache_ref, context_ref
):
    request = pl.program_id(0)
    length = length_ref[request]
    base = request * pages_of

    def order(j, carry):
        spot = place_ref[base + j]
        start = pl.multiple_of(j * page, page)
        cache_ref[0, pl.ds(start, page), :] = in_ref[
            lax.div(spot, per_block), 0, lax.rem(spot, per_block)
        ]
        return carry

    lax.fori_loop(0, pages_of, order, 0, unroll=8)
    start = pl.multiple_of(lax.div(length, page) * page, page)
    held = cache_ref[0, pl.ds(start, page), :]
    row = lax.broadcasted_iota(jnp.int32, held.shape, 0)
    fresh = jnp.broadcast_to(fresh_ref[0].astype(jnp.float32), held.shape)
    cache_ref[0, pl.ds(start, page), :] = jnp.where(
        row == lax.rem(length, page), fresh, held.astype(jnp.float32)
    ).astype(held.dtype)
    keys = cache_ref[0, :, :head_dim]
    values = cache_ref[0, :, head_dim:]
    scores = lax.dot_general(
        query_ref[0], keys, (((1,), (1,)), ((), ())), preferred_element_type=jnp.float32
    ) * head_dim ** (-0.5)
    seen = lax.broadcasted_iota(jnp.int32, scores.shape, 1) <= length
    peak = jnp.max(jnp.where(seen, scores, -jnp.inf), axis=1, keepdims=True)
    weights = jnp.where(seen, jnp.exp(scores - peak), 0.0)
    probs = (weights / jnp.sum(weights, axis=1, keepdims=True)).astype(jnp.bfloat16)
    context_ref[0] = jnp.dot(probs, values, preferred_element_type=jnp.float32).astype(
        context_ref.dtype
    )


def attend(arrived, place, lengths, fresh, query, head_dim):
    blocks, rows, per_block, page, width = arrived.shape
    pages_of = blocks * per_block
    heads = query.shape[1]
    return pl.pallas_call(
        functools.partial(attend_kernel, pages_of, per_block, page, head_dim),
        out_shape=(
            jax.ShapeDtypeStruct((rows, pages_of * page, width), arrived.dtype),
            jax.ShapeDtypeStruct(query.shape, jnp.bfloat16),
        ),
        grid_spec=pltpu.PrefetchScalarGridSpec(
            num_scalar_prefetch=2,
            grid=(rows,),
            in_specs=[
                pl.BlockSpec((blocks, 1, per_block, page, width), lambda r, *_: (0, r, 0, 0, 0)),
                pl.BlockSpec((1, 1, width), lambda r, *_: (r, 0, 0)),
                pl.BlockSpec((1, heads, head_dim), lambda r, *_: (r, 0, 0)),
            ],
            out_specs=(
                pl.BlockSpec((1, pages_of * page, width), lambda r, *_: (r, 0, 0)),
                pl.BlockSpec((1, heads, head_dim), lambda r, *_: (r, 0, 0)),
            ),
        ),
        cost_estimate=pl.CostEstimate(
            flops=4 * rows * heads * pages_of * page * head_dim,
            bytes_accessed=4 * arrived.size,
            transcendentals=rows * heads * pages_of * page,
        ),
        compiler_params=pltpu.CompilerParams(vmem_limit_bytes=40 * 2**20),
        name="attend",
    )(place.reshape(-1), lengths, arrived, fresh[:, None, :], query)


def shards(hidden_state, norm_gain, wq_old, wkv_old, kv_old, page_table, lengths):
    sections = lax.axis_size("section")
    tensors = lax.axis_size("tensor")
    section_id = lax.axis_index("section")
    tensor_id = lax.axis_index("tensor")
    rows = hidden_state.shape[0]
    head_dim = HEAD_DIM
    width = 2 * head_dim
    repeats = tensors // KV_HEADS
    queries_here = wq_old.shape[1] // head_dim
    pool_dev = kv_old.shape[1]
    page = kv_old.shape[2]
    per_block = page_table.shape[1] // tensors
    widened = hidden_state.astype(jnp.float32)
    scale = lax.rsqrt(jnp.mean(widened * widened, axis=1, keepdims=True) + EPSILON)
    normed = (widened * scale * norm_gain[None, :]).astype(jnp.bfloat16)
    owner = page_table // pool_dev
    blocks = jnp.arange(tensors, dtype=jnp.int32)
    onehot = (owner[:, :, None] == blocks[None, None, :]).astype(jnp.int32)
    ranks = jnp.sum((jnp.cumsum(onehot, axis=1) - 1) * onehot, axis=2)
    mine = owner == tensor_id
    wanted = ranks[:, :, None] == jnp.arange(per_block, dtype=jnp.int32)[None, None, :]
    picks = (mine[:, :, None] & wanted).astype(jnp.int32)
    spots = jnp.sum(picks * (page_table % pool_dev)[:, :, None], axis=1)
    pages = pick_pages(kv_old, spots.reshape(-1), sections)
    query, arrived, wkv_new, wq_new, _, _ = exchange(
        normed, wq_old, pages, wkv_old, sections, tensors, repeats
    )
    arrived = arrived.reshape(tensors, rows, per_block, page, width)
    place = lax.dynamic_slice_in_dim(owner * per_block + ranks, section_id * rows, rows, 0)
    my_lengths = lax.dynamic_slice_in_dim(lengths, section_id * rows, rows, 0)
    fresh = jnp.dot(normed, wkv_new, preferred_element_type=jnp.float32)
    fresh_key = rotate(fresh[:, None, :head_dim], my_lengths, head_dim)[:, 0]
    fresh = jnp.concatenate([fresh_key, fresh[:, head_dim:]], axis=1).astype(jnp.bfloat16)
    query = rotate(query.reshape(rows, queries_here, head_dim), my_lengths, head_dim).astype(
        jnp.bfloat16
    )
    cache, context = attend(arrived, place, my_lengths, fresh, query, head_dim)
    return (context.reshape(rows, queries_here * head_dim), cache[:, None], wq_new, wkv_new)


def solution(mesh):
    placed = (
        P("section", None),
        P(),
        P("section", "tensor"),
        P("tensor", "section"),
        P("section", "tensor", None, None),
        P(),
        P(),
    )
    return jax.shard_map(
        shards,
        mesh=mesh,
        in_specs=placed,
        out_specs=(
            P("section", "tensor"),
            P("section", "tensor", None, None),
            P(None, "tensor"),
            P(None, "tensor"),
        ),
        check_vma=False,
    )
```
